32 devices in a mesh: rep: 4 (over y, core), site: 8 (over z, x).
Axes of the slice: x: 2, y: 2, z: 4, core: 2. Of those that a mesh axis runs over, the one named last changes fastest.
Arguments:
- working: bfloat16 [4, 8, 16, 64, 2304], P('rep', 'site'), may hold values from -4 to 4
- master_slots: float32 [8, 4, 4, 64, 2304], P('site', 'rep'), may hold values from -4 to 4
- accum_slots: float32 [8, 4, 4, 64, 2304], P('site', 'rep'), may hold values from 0.01 to 1
- pool_images: bfloat16 [4, 256, 8, 1024], P(None, None, 'site'), may hold values from -6 to 6
- pool_targets: bfloat16 [4, 8, 16, 64, 256], P(None, 'site'), may hold values from -0.8984375 to 0.8984375
- batch_index: int32 [4, 3], replicated, may hold values from 0 to 3
- owner_map: int32 [4], replicated, may hold values from 0 to 3, each once
Outputs:
- working_next: bfloat16 [8, 16, 64, 2304], P('site')
- master_next: float32 [8, 4, 4, 64, 2304], P('site', 'rep')
- accum_next: float32 [8, 4, 4, 64, 2304], P('site', 'rep')
The draws below stay inside these ranges and needn't reach their ends.
Inputs may be any that keep to these rules, and one draw needn't show every extreme that they name: `owner_map`: each replica owns exactly one shard.
All inputs are finite; a program needn't handle non-finite values.
Results may differ from the reference program's by a relative error of at most 0.015.
Values may be sent and summed in bfloat16 or wider, within the bound.
No kernel may reach another device: no remote copies, remote signals or barrier semaphores. Data moves between devices by JAX's collectives and lax.ppermute only.
A program may use at most 192 MiB of HBM per device.

```python
import math
import jax
import jax.numpy as jnp
from jax import lax

MAPS = 64
CHANNELS = 64
FIELD = 6
SCOLS = 16
BATCH = 256
MICRO = 3
POOL = 4
ROWS = 8
KDIM = 2304
CB = 4
N_REP = 4


def touch_ends(result, own_key, least, largest):
    dims = result.shape
    spot = [jax.random.randint(jax.random.fold_in(own_key, axis), (), 0, dims[axis]) for axis in range(len(dims))]
    result = result.at[tuple(spot)].set(least)
    longest = dims.index(max(dims))
    spot[longest] = (spot[longest] + 1) % dims[longest]
    return result.at[tuple(spot)].set(largest)


def steps_of(rng, extent, shards, smallest, largest):
    factor_of = 1.0
    for axis_at, shards_of in shards:
        heights = jax.random.uniform(jax.random.fold_in(jax.random.fold_in(rng, 6), axis_at), (shards_of,), jnp.float32, smallest / len(shards), largest / len(shards))
        factor_of = factor_of * jnp.repeat(jnp.exp(heights), extent[axis_at] // shards_of).reshape((-1,) + (1,) * (len(extent) - 1 - axis_at))
    return factor_of


def scatter_about(rng, extent, deviation, limit, cuts=(), kind=jnp.bfloat16):
    values = deviation * jax.random.normal(rng, extent, jnp.float32)
    if cuts:
        values = values * steps_of(rng, extent, cuts, -0.22, 0.18)
    return jnp.clip(values, -limit, limit).astype(kind)


def setup_inputs(seed: int = 0) -> dict:
    seeds = jax.random.split(jax.random.key(seed), 8)
    working = scatter_about(seeds[0], (N_REP, ROWS, SCOLS, MAPS, KDIM), 1.0, 4.0, ((0, 4), (1, 8)))
    master_slots = scatter_about(seeds[1], (ROWS, N_REP, CB, MAPS, KDIM), 1.0, 4.0, ((0, 8), (1, 4)), jnp.float32)
    accum_slots = jnp.clip(jnp.exp(math.log(1.0) - 4.6051702 * jax.random.uniform(seeds[2], (ROWS, N_REP, CB, MAPS, KDIM), jnp.float32) ** steps_of(seeds[2], (ROWS, N_REP, CB, MAPS, KDIM), ((0, 8), (1, 4)), -0.2, 0.2)), 0.01, 1.0)
    pool_images = scatter_about(seeds[3], (POOL, BATCH, ROWS, SCOLS * CHANNELS), 1.0, 6.0, ((2, 8),))
    pool_targets = jnp.clip(jax.random.uniform(seeds[4], (POOL, ROWS, SCOLS, MAPS, BATCH), jnp.float32, -0.8984375, 0.8984375) * steps_of(seeds[4], (POOL, ROWS, SCOLS, MAPS, BATCH), ((1, 8),), -0.4, 0.0), -0.8984375, 0.8984375).astype(jnp.bfloat16)
    batch_index = touch_ends(jax.random.randint(seeds[5], (N_REP, MICRO), 0, POOL), jax.random.fold_in(seeds[5], 1), 0, POOL - 1).astype(jnp.int32)
    owner_map = jax.random.permutation(seeds[6], N_REP).astype(jnp.int32)
    return dict(working=working, master_slots=master_slots, accum_slots=accum_slots, pool_images=pool_images, pool_targets=pool_targets, batch_index=batch_index, owner_map=owner_map)


learning_rate = 0.3
epsilon = 1e-08

def build_patches(window):
    batch_rows = window.shape[0]
    columns = window.shape[2] // CHANNELS
    grid_cells = window.reshape(batch_rows, FIELD, columns, CHANNELS)
    padded = jnp.pad(grid_cells, ((0, 0), (0, 0), (2, 3), (0, 0)))
    stacked = jnp.stack([padded[:, :, offset:offset + columns, :] for offset in range(FIELD)], axis=2)
    return stacked.transpose(0, 3, 1, 2, 4).reshape(batch_rows, columns, FIELD * FIELD * CHANNELS)

def replica_gradient(weights, chosen, pool_images, pool_targets):
    factor = (FIELD * FIELD * CHANNELS) ** (-0.5)
    total = jnp.zeros(weights.shape, jnp.float32)
    for micro_step in range(MICRO):
        images = lax.dynamic_index_in_dim(pool_images, chosen[micro_step], 0, keepdims=False)
        targets = lax.dynamic_index_in_dim(pool_targets, chosen[micro_step], 0, keepdims=False)
        padded = jnp.pad(images, ((0, 0), (2, 3), (0, 0)))

        def row_gradient(site_row):
            window = lax.dynamic_slice_in_dim(padded, site_row, FIELD, 1)
            patches = build_patches(window).astype(jnp.float32)
            row_weights = lax.dynamic_index_in_dim(weights, site_row, 0, keepdims=False).astype(jnp.float32)
            row_targets = lax.dynamic_index_in_dim(targets, site_row, 0, keepdims=False).astype(jnp.float32)
            forward = factor * jnp.einsum('bck,cok->cob', patches, row_weights)
            active = jnp.tanh(forward)
            signal = ((active - row_targets) * (1.0 - active * active)).astype(jnp.bfloat16)
            signal = lax.optimization_barrier(signal).astype(jnp.float32)
            return factor * jnp.einsum('cob,bck->cok', signal, patches)
        total = total + lax.map(row_gradient, jnp.arange(ROWS, dtype=jnp.int32))
    return total

def reference(working, master_slots, accum_slots, pool_images, pool_targets, batch_index, owner_map):
    total = jnp.zeros((ROWS, SCOLS, MAPS, FIELD * FIELD * CHANNELS), jnp.float32)
    for replica in range(N_REP):
        partial_grad = replica_gradient(working[replica], batch_index[replica], pool_images, pool_targets)
        rounded = lax.optimization_barrier(partial_grad.astype(jnp.bfloat16))
        total = total + rounded.astype(jnp.float32)
    blocks = total.reshape(ROWS, N_REP, SCOLS // N_REP, MAPS, FIELD * FIELD * CHANNELS)
    slot_grad = jnp.take(blocks, owner_map, axis=1)
    accum_next = accum_slots + slot_grad * slot_grad
    master_next = master_slots - learning_rate * slot_grad / (jnp.sqrt(accum_next) + epsilon)
    numbers = jnp.arange(N_REP, dtype=jnp.int32)
    matches = (owner_map[:, None] == numbers[None, :]).astype(jnp.int32)
    inverse = lax.optimization_barrier(jnp.sum(numbers[:, None] * matches, axis=0))
    working_next = jnp.take(master_next.astype(jnp.bfloat16), inverse, axis=1)
    working_next = working_next.reshape(ROWS, SCOLS, MAPS, FIELD * FIELD * CHANNELS)
    return (working_next, master_next, accum_next)
```

```python
import functools

import jax
import jax.numpy as jnp
from jax import lax
from jax.experimental import pallas as pl
from jax.experimental.pallas import tpu as pltpu
from jax.sharding import PartitionSpec as P

FIELD = 6
BEFORE = 2
MICRO = 3

learning_rate = 0.3
epsilon = 1e-08

ANY = pl.BlockSpec(memory_space=pl.ANY)
SMEM = pl.BlockSpec(memory_space=pltpu.SMEM)
VMEM_LIMIT = 56 * 1024 * 1024


def moved(x, axis, target):
    n = lax.axis_size(axis)
    pairs = [(i, target(i)) for i in range(n)]
    return lax.ppermute(x, axis, [(i, t) for i, t in pairs if t is not None and 0 <= t < n])


def sizes_of(geo):
    maps, cols, block, channels = geo
    window = -(-(block + FIELD - 1) * channels // 128) * 128
    return maps, cols, block, channels, window


def window_cases(geo):
    maps, cols, block, channels, window = sizes_of(geo)
    cases = []
    for shard in range(cols // block):
        first = shard * block * channels - BEFORE * channels
        lo, hi = max(first, 0), min(first + window, cols * channels)
        cases.append((lo, hi - lo, lo - first))
    return cases


def load_rows(info, geo, drs, near, own, dst, sem):
    window = sizes_of(geo)[-1]
    half = own.shape[0] // 2
    shard, odd, core = info[0], info[1], info[2]
    here, there = core * half, (1 - core) * half

    def both(case, at, pair):
        lo, width, to = case
        dst_lanes = pl.ds(at + to, width)
        for start, ref in zip((here, there), pair):
            pltpu.make_async_copy(
                ref.at[:, :, pl.ds(lo, width)], dst.at[pl.ds(start, half), :, dst_lanes], sem
            ).start()

    for number, case in enumerate(window_cases(geo)):

        @pl.when(shard == number)
        def _(case=case):
            lo, width, to = case
            for place, dr in enumerate(drs):
                at = place * window
                if dr == BEFORE:
                    pltpu.make_async_copy(
                        own.at[:, :, pl.ds(lo, width)], dst.at[:, :, pl.ds(at + to, width)], sem
                    ).start()
                    continue
                even_pair, odd_pair = near[dr]
                if even_pair is odd_pair:
                    both(case, at, even_pair)
                else:

                    @pl.when(odd == 0)
                    def _():
                        both(case, at, even_pair)

                    @pl.when(odd == 1)
                    def _():
                        both(case, at, odd_pair)


def wait_rows(info, geo, drs, dst, sem):
    for number, (_, width, _) in enumerate(window_cases(geo)):

        @pl.when(info[0] == number)
        def _(width=width):
            taken = dst.at[:, :, pl.ds(0, len(drs) * width)]
            pltpu.make_async_copy(taken, taken, sem).wait()


def clear_edges(geo, drs, dst):
    window = sizes_of(geo)[-1]
    zero_lanes = set()
    for lo, width, to in window_cases(geo):
        zero_lanes |= set(range(0, to, 128)) | set(range(to + width, window, 128))
    for place in range(len(drs)):
        for lane in sorted(zero_lanes):
            dst[:, :, place * window + lane : place * window + lane + 128] = jnp.zeros(
                dst.shape[:2] + (128,), dst.dtype
            )


def band(geo, drs, weights, wide):
    maps, cols, block, channels, window = sizes_of(geo)
    span = FIELD * channels
    for place in range(len(drs)):
        for p in range(block):
            w = weights[p, :, place * span : (place + 1) * span]
            parts = []
            if p:
                parts.append(jnp.zeros((maps, p * channels), w.dtype))
            parts.append(w)
            parts.append(jnp.zeros((maps, window - span - p * channels), w.dtype))
            wide[p * maps : (p + 1) * maps, place * window : (place + 1) * window] = (
                jnp.concatenate(parts, axis=1)
            )


NT = (((1,), (1,)), ((), ()))


def forward_kernel(geo, drs, last, n_near, factor, *refs):
    info, choice = refs[0], refs[1]
    own = refs[2]
    flat = refs[3 : 3 + n_near]
    w_refs = refs[3 + n_near : 7 + n_near]
    rest = refs[7 + n_near :]
    if last:
        before, targets, out, xs, wb, wide, tb, pb, sem, wsem, tsem = rest
    else:
        out, xs, wb, wide, sem, wsem = rest
    near = unflatten(drs, flat)
    maps, cols, block, channels, window = sizes_of(geo)
    span = FIELD * channels
    lanes = pl.ds(drs[0] * span, len(drs) * span)
    copies = []
    for k in range(4):
        if k == 0:
            src = w_refs[0].at[pl.ds(info[0] * block, block), :, lanes]
        else:
            src = w_refs[k].at[:, :, lanes]
        copies.append(pltpu.make_async_copy(src, wb.at[k], wsem.at[k]))
        copies[-1].start()
    if last:
        t_copy = pltpu.make_async_copy(
            targets.at[:, pl.ds(info[0] * block * maps, block * maps), :], tb, tsem.at[0]
        )
        p_copy = pltpu.make_async_copy(before, pb, tsem.at[1])
        t_copy.start()
        p_copy.start()
    clear_edges(geo, drs, xs)
    load_rows(info, geo, drs, near, own, xs, sem)
    for c in copies:
        c.wait()
    if last:
        t_copy.wait()
        p_copy.wait()
    wait_rows(info, geo, drs, xs, sem)

    def per_replica(k, carry):
        band(geo, drs, wb.at[k], wide)

        def per_step(m, carry):
            q = choice[k * MICRO + m]
            pre = lax.dot_general(wide[...], xs[q], NT, preferred_element_type=jnp.float32)
            at = k * MICRO + m
            if last:
                act = jnp.tanh(factor * (pre + pb[at]))
                sig = (act - tb[q].astype(jnp.float32)) * (1.0 - act * act)
                out[at] = sig.astype(out.dtype)
            else:
                out[at] = pre
            return carry

        return lax.fori_loop(0, MICRO, per_step, carry)

    lax.fori_loop(0, 4, per_replica, 0)


def backward_kernel(geo, drs, n_near, n_alias, factor, *refs):
    info, choice, own = refs[0], refs[1], refs[2]
    flat = refs[3 : 3 + n_near]
    sig, master, accum = refs[3 + n_near : 6 + n_near]
    rest = refs[6 + n_near + n_alias :]
    shard_out, master_out, accum_out, xs, total, sem = rest
    near = unflatten(drs, flat)
    maps, cols, block, channels, window = sizes_of(geo)
    span = FIELD * channels
    clear_edges(geo, drs, xs)
    load_rows(info, geo, drs, near, own, xs, sem)
    wait_rows(info, geo, drs, xs, sem)
    total[...] = jnp.zeros_like(total)

    def per_replica(k, carry):
        acc = None
        for m in range(MICRO):
            q = choice[k * MICRO + m]
            part = jnp.dot(sig[k * MICRO + m], xs[q], preferred_element_type=jnp.float32)
            acc = part if acc is None else acc + part
        total[...] += (factor * acc).astype(jnp.bfloat16).astype(jnp.float32)
        return carry

    lax.fori_loop(0, 4, per_replica, 0)
    for place in range(len(drs)):
        for p in range(block):
            at = place * window + p * channels
            slot = total[p * maps : (p + 1) * maps, at : at + span]
            here = slice(place * span, (place + 1) * span)
            grown = accum[p, :, here] + slot * slot
            new = master[p, :, here] - learning_rate * slot / (jnp.sqrt(grown) + epsilon)
            accum_out[p, :, here] = grown
            master_out[p, :, here] = new
            shard_out[p, :, here] = new.astype(jnp.bfloat16)


def near_for(drs, rows):
    flat = []
    for dr in drs:
        if dr != BEFORE:
            even_pair, odd_pair = rows[dr]
            flat += list(even_pair)
            if odd_pair is not even_pair:
                flat += list(odd_pair)
    return flat


TWO_SOURCES = (1, 3, 5)


def unflatten(drs, flat):
    near, at = {}, 0
    for dr in drs:
        if dr == BEFORE:
            continue
        even_pair = (flat[at], flat[at + 1])
        at += 2
        odd_pair = even_pair
        if dr in TWO_SOURCES:
            odd_pair = (flat[at], flat[at + 1])
            at += 2
        near[dr] = (even_pair, odd_pair)
    return near


def forward(geo, drs, factor, info, choice, own, rows, w_blocks, before=None, targets=None):
    maps, cols, block, channels, window = sizes_of(geo)
    pool, batch, _ = own.shape
    flat = near_for(drs, rows)
    last = before is not None
    tall = block * maps
    scratch = [
        pltpu.VMEM((pool, batch, len(drs) * window), own.dtype),
        pltpu.VMEM((4, block, maps, len(drs) * FIELD * channels), own.dtype),
        pltpu.VMEM((tall, len(drs) * window), own.dtype),
    ]
    inputs = [info, choice, own, *flat, *w_blocks]
    if last:
        scratch += [
            pltpu.VMEM((pool, tall, batch), targets.dtype),
            pltpu.VMEM((4 * MICRO, tall, batch), jnp.float32),
        ]
        inputs += [before, targets]
    scratch += [pltpu.SemaphoreType.DMA, pltpu.SemaphoreType.DMA((4,))]
    if last:
        scratch += [pltpu.SemaphoreType.DMA((2,))]
    return pl.pallas_call(
        functools.partial(forward_kernel, geo, drs, last, len(flat), factor),
        out_shape=jax.ShapeDtypeStruct(
            (4 * MICRO, tall, batch), own.dtype if last else jnp.float32
        ),
        in_specs=[SMEM, SMEM] + [ANY] * (len(inputs) - 2),
        out_specs=pl.BlockSpec(memory_space=pltpu.VMEM),
        scratch_shapes=scratch,
        compiler_params=pltpu.CompilerParams(vmem_limit_bytes=VMEM_LIMIT),
        cost_estimate=pl.CostEstimate(
            flops=2 * 12 * tall * batch * len(drs) * window, transcendentals=0, bytes_accessed=8 << 20
        ),
        name="forward",
    )(*inputs)


def backward(geo, drs, factor, info, choice, own, rows, sig, master, accum, outs):
    maps, cols, block, channels, window = sizes_of(geo)
    pool, batch, _ = own.shape
    span = FIELD * channels
    flat = near_for(drs, rows)
    tall = block * maps
    j = drs[0] // len(drs)
    lanes = pl.BlockSpec((block, maps, len(drs) * span), lambda i: (0, 0, j))
    n_in = 3 + len(flat) + 3
    n_alias = 0 if outs is None else 2
    whole = jax.ShapeDtypeStruct(master.shape, jnp.float32)
    return pl.pallas_call(
        functools.partial(backward_kernel, geo, drs, len(flat), n_alias, factor),
        grid=(1,),
        out_shape=(
            jax.ShapeDtypeStruct((block, maps, len(drs) * span), jnp.bfloat16),
            whole,
            whole,
        ),
        in_specs=[SMEM, SMEM]
        + [ANY] * (1 + len(flat))
        + [pl.BlockSpec(sig.shape, lambda i: (0, 0, 0)), lanes, lanes]
        + [ANY] * n_alias,
        out_specs=(
            pl.BlockSpec((block, maps, len(drs) * span), lambda i: (0, 0, 0)),
            lanes,
            lanes,
        ),
        input_output_aliases={} if outs is None else {n_in: 1, n_in + 1: 2},
        scratch_shapes=[
            pltpu.VMEM((pool, batch, len(drs) * window), own.dtype),
            pltpu.VMEM((tall, len(drs) * window), jnp.float32),
            pltpu.SemaphoreType.DMA,
        ],
        compiler_params=pltpu.CompilerParams(vmem_limit_bytes=VMEM_LIMIT),
        cost_estimate=pl.CostEstimate(
            flops=2 * 12 * tall * batch * len(drs) * window, transcendentals=0, bytes_accessed=8 << 20
        ),
        name="backward",
    )(info, choice, own, *flat, sig, master, accum, *(outs or ()))


def place_kernel(first_lane, block, shards, *refs):
    a = refs[1:5]
    out, sem = refs[-2:]
    copies = [
        pltpu.make_async_copy(
            a[k],
            out.at[pl.ds(refs[0][k] * block, block), :, pl.ds(first_lane, a[k].shape[2])],
            sem.at[k],
        )
        for k in range(4)
    ]
    for c in copies:
        c.start()
    for c in copies:
        c.wait()


def place(shards, pieces, first_lane, shape, out):
    block = pieces[0].shape[0]
    extra = [] if out is None else [out]
    return pl.pallas_call(
        functools.partial(place_kernel, first_lane, block, 4),
        out_shape=jax.ShapeDtypeStruct(shape, jnp.bfloat16),
        in_specs=[SMEM] + [ANY] * (4 + len(extra)),
        out_specs=ANY,
        input_output_aliases={5: 0} if extra else {},
        scratch_shapes=[pltpu.SemaphoreType.DMA((4,))],
        name="place",
    )(shards, *pieces, *extra)


def per_device(
    working, master_slots, accum_slots, pool_images, pool_targets, batch_index, owner_map
):
    rep = lax.axis_index("rep")
    site = lax.axis_index("site")
    replicas = lax.axis_size("rep")
    weights = working[0, 0]
    cols, maps, depth = weights.shape
    factor = depth ** (-0.5)
    block = cols // replicas
    pool, batch, _, lanes = pool_images.shape
    geo = (maps, cols, block, lanes // cols)
    own = pool_images.reshape(pool, batch, lanes)
    targets = pool_targets.reshape(pool, cols * maps, batch)
    peers = [rep ^ k for k in range(replicas)]
    shards = jnp.stack([owner_map[p] for p in peers]).astype(jnp.int32)
    choice = jnp.concatenate([batch_index[p] for p in peers]).astype(jnp.int32)
    core = rep % 2
    info = jnp.stack([shards[0], site % 2, core]).astype(jnp.int32)

    half = lax.dynamic_slice_in_dim(own, core * (pool // 2), pool // 2, 0)
    beside = moved(half, "site", lambda i: i ^ 1)
    from_before = moved(half, "site", lambda i: i + 2)
    from_after = moved(half, "site", lambda i: i - 2)
    w_blocks = [weights]
    for k in range(1, replicas):
        piece = lax.dynamic_slice_in_dim(weights, shards[k] * block, block, 0)
        w_blocks.append(moved(piece, "rep", lambda i, k=k: i ^ k))
    further_before = moved(beside, "site", lambda i: i + 2 if i % 2 == 0 else None)
    further_after = moved(beside, "site", lambda i: i - 2)
    last_after = moved(from_after, "site", lambda i: i - 1 if i % 2 == 0 else None)

    def pair(x):
        return (x, moved(x, "rep", lambda i: i ^ 1))

    beside, from_before, from_after, further_before, further_after, last_after = [
        pair(x)
        for x in (beside, from_before, from_after, further_before, further_after, last_after)
    ]
    rows = {
        0: (from_before, from_before),
        1: (further_before, beside),
        3: (beside, further_after),
        4: (from_after, from_after),
        5: (further_after, last_after),
    }
    partial = forward(geo, (0, 1, 2, 3, 4), factor, info, choice, own, rows, w_blocks)
    signal = forward(
        geo, (5,), factor, info, choice, own, rows, w_blocks, partial, targets
    )
    outs = None
    working_next = None
    for drs in ((0, 1), (2, 3), (4, 5)):
        fresh, *outs = backward(
            geo, drs, factor, info, choice, own, rows, signal, master_slots[0, 0], accum_slots[0, 0], outs
        )
        across = moved(fresh, "rep", lambda i: i ^ 2)
        pieces = [fresh, moved(fresh, "rep", lambda i: i ^ 1), across, moved(across, "rep", lambda i: i ^ 1)]
        working_next = place(
            shards, pieces, drs[0] * FIELD * geo[3], weights.shape, working_next
        )
    master_next, accum_next = outs
    return (working_next[None], master_next[None, None], accum_next[None, None])


def solution(mesh):
    placed = (
        P("rep", "site", None, None, None),
        P("site", "rep", None, None, None),
        P("site", "rep", None, None, None),
        P(None, None, "site", None),
        P(None, "site", None, None, None),
        P(),
        P(),
    )
    return jax.shard_map(
        per_device,
        mesh=mesh,
        in_specs=placed,
        out_specs=(
            P("site", None, None, None),
            P("site", "rep", None, None, None),
            P("site", "rep", None, None, None),
        ),
        check_vma=False,
    )
```

```python
import functools

import jax
import jax.numpy as jnp
from jax import lax
from jax.experimental import pallas as pl
from jax.experimental.pallas import tpu as pltpu
from jax.sharding import PartitionSpec as P

FIELD = 6
BEFORE = 2
MICRO = 3

learning_rate = 0.3
epsilon = 1e-08

ANY = pl.BlockSpec(memory_space=pl.ANY)
SMEM = pl.BlockSpec(memory_space=pltpu.SMEM)
VMEM_LIMIT = 56 * 1024 * 1024


def moved(x, axis, target):
    n = lax.axis_size(axis)
    pairs = [(i, target(i)) for i in range(n)]
    return lax.ppermute(x, axis, [(i, t) for i, t in pairs if t is not None and 0 <= t < n])


def sizes_of(geo):
    maps, cols, block, channels = geo
    window = -(-(block + FIELD - 1) * channels // 128) * 128
    return maps, cols, block, channels, window


def window_cases(geo):
    maps, cols, block, channels, window = sizes_of(geo)
    cases = []
    for shard in range(cols // block):
        first = shard * block * channels - BEFORE * channels
        lo, hi = max(first, 0), min(first + window, cols * channels)
        cases.append((lo, hi - lo, lo - first))
    return cases


def load_rows(info, geo, drs, near, own, dst, sem):
    window = sizes_of(geo)[-1]
    half = own.shape[0] // 2
    shard, odd, core = info[0], info[1], info[2]
    here, there = core * half, (1 - core) * half

    def both(case, at, pair):
        lo, width, to = case
        dst_lanes = pl.ds(at + to, width)
        for start, ref in zip((here, there), pair):
            pltpu.make_async_copy(
                ref.at[:, :, pl.ds(lo, width)], dst.at[pl.ds(start, half), :, dst_lanes], sem
            ).start()

    for number, case in enumerate(window_cases(geo)):

        @pl.when(shard == number)
        def _(case=case):
            lo, width, to = case
            for place, dr in enumerate(drs):
                at = place * window
                if dr == BEFORE:
                    pltpu.make_async_copy(
                        own.at[:, :, pl.ds(lo, width)], dst.at[:, :, pl.ds(at + to, width)], sem
                    ).start()
                    continue
                even_pair, odd_pair = near[dr]
                if even_pair is odd_pair:
                    both(case, at, even_pair)
                else:

                    @pl.when(odd == 0)
                    def _():
                        both(case, at, even_pair)

                    @pl.when(odd == 1)
                    def _():
                        both(case, at, odd_pair)


def wait_rows(info, geo, drs, dst, sem):
    for number, (_, width, _) in enumerate(window_cases(geo)):

        @pl.when(info[0] == number)
        def _(width=width):
            taken = dst.at[:, :, pl.ds(0, len(drs) * width)]
            pltpu.make_async_copy(taken, taken, sem).wait()


def clear_edges(geo, drs, dst):
    window = sizes_of(geo)[-1]
    zero_lanes = set()
    for lo, width, to in window_cases(geo):
        zero_lanes |= set(range(0, to, 128)) | set(range(to + width, window, 128))
    for place in range(len(drs)):
        for lane in sorted(zero_lanes):
            dst[:, :, place * window + lane : place * window + lane + 128] = jnp.zeros(
                dst.shape[:2] + (128,), dst.dtype
            )


def band(geo, drs, weights, wide):
    maps, cols, block, channels, window = sizes_of(geo)
    span = FIELD * channels
    for place in range(len(drs)):
        for p in range(block):
            w = weights[p, :, place * span : (place + 1) * span]
            parts = []
            if p:
                parts.append(jnp.zeros((maps, p * channels), w.dtype))
            parts.append(w)
            parts.append(jnp.zeros((maps, window - span - p * channels), w.dtype))
            wide[p * maps : (p + 1) * maps, place * window : (place + 1) * window] = (
                jnp.concatenate(parts, axis=1)
            )


NT = (((1,), (1,)), ((), ()))


def forward_kernel(geo, drs, last, n_near, factor, *refs):
    info, choice = refs[0], refs[1]
    own = refs[2]
    flat = refs[3 : 3 + n_near]
    w_refs = refs[3 + n_near : 7 + n_near]
    rest = refs[7 + n_near :]
    if last:
        before, targets, out, xs, wb, wide, tb, pb, sem, wsem, tsem = rest
    else:
        out, xs, wb, wide, sem, wsem = rest
    near = unflatten(drs, flat)
    maps, cols, block, channels, window = sizes_of(geo)
    span = FIELD * channels
    lanes = pl.ds(drs[0] * span, len(drs) * span)
    copies = []
    for k in range(4):
        if k == 0:
            src = w_refs[0].at[pl.ds(info[0] * block, block), :, lanes]
        else:
            src = w_refs[k].at[:, :, lanes]
        copies.append(pltpu.make_async_copy(src, wb.at[k], wsem.at[k]))
        copies[-1].start()
    if last:
        t_copy = pltpu.make_async_copy(
            targets.at[:, pl.ds(info[0] * block * maps, block * maps), :], tb, tsem.at[0]
        )
        p_copy = pltpu.make_async_copy(before, pb, tsem.at[1])
        t_copy.start()
        p_copy.start()
    clear_edges(geo, drs, xs)
    load_rows(info, geo, drs, near, own, xs, sem)
    for c in copies:
        c.wait()
    if last:
        t_copy.wait()
        p_copy.wait()
    wait_rows(info, geo, drs, xs, sem)

    def per_replica(k, carry):
        band(geo, drs, wb.at[k], wide)

        def per_step(m, carry):
            q = choice[k * MICRO + m]
            pre = lax.dot_general(wide[...], xs[q], NT, preferred_element_type=jnp.float32)
            at = k * MICRO + m
            if last:
                act = jnp.tanh(factor * (pre + pb[at]))
                sig = (act - tb[q].astype(jnp.float32)) * (1.0 - act * act)
                out[at] = sig.astype(out.dtype)
            else:
                out[at] = pre
            return carry

        return lax.fori_loop(0, MICRO, per_step, carry)

    lax.fori_loop(0, 4, per_replica, 0)


def backward_kernel(geo, drs, n_near, n_alias, factor, *refs):
    info, choice, own = refs[0], refs[1], refs[2]
    flat = refs[3 : 3 + n_near]
    sig, master, accum = refs[3 + n_near : 6 + n_near]
    rest = refs[6 + n_near + n_alias :]
    shard_out, master_out, accum_out, xs, total, sem = rest
    near = unflatten(drs, flat)
    maps, cols, block, channels, window = sizes_of(geo)
    span = FIELD * channels
    clear_edges(geo, drs, xs)
    load_rows(info, geo, drs, near, own, xs, sem)
    wait_rows(info, geo, drs, xs, sem)
    total[...] = jnp.zeros_like(total)

    def per_replica(k, carry):
        acc = None
        for m in range(MICRO):
            q = choice[k * MICRO + m]
            part = jnp.dot(sig[k * MICRO + m], xs[q], preferred_element_type=jnp.float32)
            acc = part if acc is None else acc + part
        total[...] += (factor * acc).astype(jnp.bfloat16).astype(jnp.float32)
        return carry

    lax.fori_loop(0, 4, per_replica, 0)
    for place in range(len(drs)):
        for p in range(block):
            at = place * window + p * channels
            slot = total[p * maps : (p + 1) * maps, at : at + span]
            here = slice(place * span, (place + 1) * span)
            grown = accum[p, :, here] + slot * slot
            new = master[p, :, here] - learning_rate * slot / (jnp.sqrt(grown) + epsilon)
            accum_out[p, :, here] = grown
            master_out[p, :, here] = new
            shard_out[p, :, here] = new.astype(jnp.bfloat16)


def near_for(drs, rows):
    flat = []
    for dr in drs:
        if dr != BEFORE:
            even_pair, odd_pair = rows[dr]
            flat += list(even_pair)
            if odd_pair is not even_pair:
                flat += list(odd_pair)
    return flat


TWO_SOURCES = (1, 3, 5)


def unflatten(drs, flat):
    near, at = {}, 0
    for dr in drs:
        if dr == BEFORE:
            continue
        even_pair = (flat[at], flat[at + 1])
        at += 2
        odd_pair = even_pair
        if dr in TWO_SOURCES:
            odd_pair = (flat[at], flat[at + 1])
            at += 2
        near[dr] = (even_pair, odd_pair)
    return near


def forward(geo, drs, factor, info, choice, own, rows, w_blocks, before=None, targets=None):
    maps, cols, block, channels, window = sizes_of(geo)
    pool, batch, _ = own.shape
    flat = near_for(drs, rows)
    last = before is not None
    tall = block * maps
    scratch = [
        pltpu.VMEM((pool, batch, len(drs) * window), own.dtype),
        pltpu.VMEM((4, block, maps, len(drs) * FIELD * channels), own.dtype),
        pltpu.VMEM((tall, len(drs) * window), own.dtype),
    ]
    inputs = [info, choice, own, *flat, *w_blocks]
    if last:
        scratch += [
            pltpu.VMEM((pool, tall, batch), targets.dtype),
            pltpu.VMEM((4 * MICRO, tall, batch), jnp.float32),
        ]
        inputs += [before, targets]
    scratch += [pltpu.SemaphoreType.DMA, pltpu.SemaphoreType.DMA((4,))]
    if last:
        scratch += [pltpu.SemaphoreType.DMA((2,))]
    return pl.pallas_call(
        functools.partial(forward_kernel, geo, drs, last, len(flat), factor),
        out_shape=jax.ShapeDtypeStruct(
            (4 * MICRO, tall, batch), own.dtype if last else jnp.float32
        ),
        in_specs=[SMEM, SMEM] + [ANY] * (len(inputs) - 2),
        out_specs=pl.BlockSpec(memory_space=pltpu.VMEM),
        scratch_shapes=scratch,
        compiler_params=pltpu.CompilerParams(vmem_limit_bytes=VMEM_LIMIT),
        cost_estimate=pl.CostEstimate(
            flops=2 * 12 * tall * batch * len(drs) * window, transcendentals=0, bytes_accessed=8 << 20
        ),
        name="forward",
    )(*inputs)


def backward(geo, drs, factor, info, choice, own, rows, sig, master, accum, outs):
    maps, cols, block, channels, window = sizes_of(geo)
    pool, batch, _ = own.shape
    span = FIELD * channels
    flat = near_for(drs, rows)
    tall = block * maps
    j = drs[0] // len(drs)
    lanes = pl.BlockSpec((block, maps, len(drs) * span), lambda i: (0, 0, j))
    n_in = 3 + len(flat) + 3
    n_alias = 0 if outs is None else 2
    whole = jax.ShapeDtypeStruct(master.shape, jnp.float32)
    return pl.pallas_call(
        functools.partial(backward_kernel, geo, drs, len(flat), n_alias, factor),
        grid=(1,),
        out_shape=(
            jax.ShapeDtypeStruct((block, maps, len(drs) * span), jnp.bfloat16),
            whole,
            whole,
        ),
        in_specs=[SMEM, SMEM]
        + [ANY] * (1 + len(flat))
        + [pl.BlockSpec(sig.shape, lambda i: (0, 0, 0)), lanes, lanes]
        + [ANY] * n_alias,
        out_specs=(
            pl.BlockSpec((block, maps, len(drs) * span), lambda i: (0, 0, 0)),
            lanes,
            lanes,
        ),
        input_output_aliases={} if outs is None else {n_in: 1, n_in + 1: 2},
        scratch_shapes=[
            pltpu.VMEM((pool, batch, len(drs) * window), own.dtype),
            pltpu.VMEM((tall, len(drs) * window), jnp.float32),
            pltpu.SemaphoreType.DMA,
        ],
        compiler_params=pltpu.CompilerParams(vmem_limit_bytes=VMEM_LIMIT),
        cost_estimate=pl.CostEstimate(
            flops=2 * 12 * tall * batch * len(drs) * window, transcendentals=0, bytes_accessed=8 << 20
        ),
        name="backward",
    )(info, choice, own, *flat, sig, master, accum, *(outs or ()))


def place_kernel(first_lane, block, *refs):
    a = refs[1:5]
    out, held, in_sem, out_sem = refs[-4:]
    takes = [pltpu.make_async_copy(a[k], held.at[k], in_sem.at[k]) for k in range(4)]
    puts = [
        pltpu.make_async_copy(
            held.at[k],
            out.at[pl.ds(refs[0][k] * block, block), :, pl.ds(first_lane, a[k].shape[2])],
            out_sem.at[k],
        )
        for k in range(4)
    ]
    for take in takes:
        take.start()
    for take, put in zip(takes, puts):
        take.wait()
        put.start()
    for put in puts:
        put.wait()


def place(shards, pieces, first_lane, shape, out):
    block = pieces[0].shape[0]
    extra = [] if out is None else [out]
    return pl.pallas_call(
        functools.partial(place_kernel, first_lane, block),
        out_shape=jax.ShapeDtypeStruct(shape, jnp.bfloat16),
        in_specs=[SMEM] + [ANY] * (4 + len(extra)),
        out_specs=ANY,
        input_output_aliases={5: 0} if extra else {},
        scratch_shapes=[
            pltpu.VMEM((4,) + pieces[0].shape, jnp.bfloat16),
            pltpu.SemaphoreType.DMA((4,)),
            pltpu.SemaphoreType.DMA((4,)),
        ],
        name="place",
    )(shards, *pieces, *extra)


def per_device(
    working, master_slots, accum_slots, pool_images, pool_targets, batch_index, owner_map
):
    rep = lax.axis_index("rep")
    site = lax.axis_index("site")
    replicas = lax.axis_size("rep")
    weights = working[0, 0]
    cols, maps, depth = weights.shape
    factor = depth ** (-0.5)
    block = cols // replicas
    pool, batch, _, lanes = pool_images.shape
    geo = (maps, cols, block, lanes // cols)
    own = pool_images.reshape(pool, batch, lanes)
    targets = pool_targets.reshape(pool, cols * maps, batch)
    peers = [rep ^ k for k in range(replicas)]
    shards = jnp.stack([owner_map[p] for p in peers]).astype(jnp.int32)
    choice = jnp.concatenate([batch_index[p] for p in peers]).astype(jnp.int32)
    core = rep % 2
    info = jnp.stack([shards[0], site % 2, core]).astype(jnp.int32)

    half = lax.dynamic_slice_in_dim(own, core * (pool // 2), pool // 2, 0)
    beside = moved(half, "site", lambda i: i ^ 1)
    from_before = moved(half, "site", lambda i: i + 2)
    from_after = moved(half, "site", lambda i: i - 2)
    w_blocks = [weights]
    for k in range(1, replicas):
        piece = lax.dynamic_slice_in_dim(weights, shards[k] * block, block, 0)
        w_blocks.append(moved(piece, "rep", lambda i, k=k: i ^ k))
    further_before = moved(beside, "site", lambda i: i + 2 if i % 2 == 0 else None)
    further_after = moved(beside, "site", lambda i: i - 2)
    last_after = moved(from_after, "site", lambda i: i - 1 if i % 2 == 0 else None)

    def pair(x):
        return (x, moved(x, "rep", lambda i: i ^ 1))

    beside, from_before, from_after, further_before, further_after, last_after = [
        pair(x)
        for x in (beside, from_before, from_after, further_before, further_after, last_after)
    ]
    rows = {
        0: (from_before, from_before),
        1: (further_before, beside),
        3: (beside, further_after),
        4: (from_after, from_after),
        5: (further_after, last_after),
    }
    partial = forward(geo, (0, 1, 2, 3, 4), factor, info, choice, own, rows, w_blocks)
    signal = forward(
        geo, (5,), factor, info, choice, own, rows, w_blocks, partial, targets
    )
    outs = None
    working_next = None
    for drs in ((0, 1), (2, 3), (4, 5)):
        fresh, *outs = backward(
            geo, drs, factor, info, choice, own, rows, signal, master_slots[0, 0], accum_slots[0, 0], outs
        )
        across = moved(fresh, "rep", lambda i: i ^ 2)
        pieces = [fresh, moved(fresh, "rep", lambda i: i ^ 1), across, moved(across, "rep", lambda i: i ^ 1)]
        working_next = place(
            shards, pieces, drs[0] * FIELD * geo[3], weights.shape, working_next
        )
    master_next, accum_next = outs
    return (working_next[None], master_next[None, None], accum_next[None, None])


def solution(mesh):
    placed = (
        P("rep", "site", None, None, None),
        P("site", "rep", None, None, None),
        P("site", "rep", None, None, None),
        P(None, None, "site", None),
        P(None, "site", None, None, None),
        P(),
        P(),
    )
    return jax.shard_map(
        per_device,
        mesh=mesh,
        in_specs=placed,
        out_specs=(
            P("site", None, None, None),
            P("site", "rep", None, None, None),
            P("site", "rep", None, None, None),
        ),
        check_vma=False,
    )
```
